32 devices in a mesh: expert: 4 (over y, x), tensor: 4 (over z), rep: 2 (over core).
Axes of the slice: x: 2, y: 2, z: 4, core: 2. Of those that a mesh axis runs over, the one named last changes fastest.
Arguments:
- requests: bfloat16 [512, 1536], P('expert', ('tensor', 'rep')), may hold values from -6 to 6
- expert_ids: int32 [512, 2], P('expert'), may hold values from 0 to 3, all different within a row; in each aligned block of 128 rows (0 to 127, 128 to 255, ...) at most 96 rows name the same one
- gate_values: float32 [512, 2], P('expert'), may hold values from 0.2 to 1
- w_up: bfloat16 [4, 1536, 6144], P(None, 'expert', ('tensor', 'rep')), may hold values from -0.15625 to 0.15625
- w_down: bfloat16 [4, 1536, 6144], P(None, 'expert', ('tensor', 'rep')), may hold values from -0.078125 to 0.078125
- tower_in: bfloat16 [1536, 768], P(('tensor', 'rep')), may hold values from -0.15625 to 0.15625
- tower_bias: float32 [768], replicated, may hold values from -3 to 3
- tower_out: float32 [3, 256], replicated, may hold values from -0.375 to 0.375
- out_bias: float32 [3], replicated, may hold values from -3 to 3
Outputs:
- mixed: bfloat16 [512, 1536], P('expert', ('tensor', 'rep'))
- scores: float32 [3, 512], P(None, ('expert', 'tensor', 'rep'))
The draws below stay inside these ranges and needn't reach their ends.
Inputs may be any that keep to these rules, and one draw needn't show every extreme that they name: `expert_ids`: each row names two different experts. In the rows of one device (128 requests) no expert is named more than 96 times, a bound that some block reaches.
All inputs are finite; a program needn't handle non-finite values.
Results may differ from the reference program's by a relative error of at most 0.015.
Values may be sent and summed in bfloat16 or wider, within the bound.
No kernel may reach another device: no remote copies, remote signals or barrier semaphores. Data moves between devices by JAX's collectives and lax.ppermute only.
A program may use at most 64 MiB of HBM per device.

```python
import math
import jax
import jax.numpy as jnp
import numpy as np
from jax import lax

D = 1536
HID = 6144
TH = 256
TASKS = 3
TOK_DEV = 128
EXPERTS = 4
CAP = 96
TOKENS = 512
N_TENSOR = 4
N_REP = 2


def block_scale(key, dims, shards, smallest, largest):
    def one(position, blocks):
        steps = jax.random.uniform(jax.random.fold_in(jax.random.fold_in(key, 6), position), (blocks,), jnp.float32, smallest / len(shards), largest / len(shards))
        return jnp.repeat(jnp.exp(steps), dims[position] // blocks).reshape((-1,) + (1,) * (len(dims) - position - 1))

    loudness = one(*shards[0])
    for cut in shards[1:]:
        loudness = loudness * one(*cut)
    return loudness


def assign_block(own_key, own, number, rows, number_of, top, bound, slope):
    order = jax.random.permutation(own_key, number_of)
    packed, common = shares(number_of, rows * top, bound, slope, True), shares(number_of, rows * top, bound, slope, False)
    places = jnp.arange(number_of)

    def named(sizes, turn):
        used = int((sizes > 0).sum())
        fixed = max(1, used // 4)
        moved = fixed + (places - fixed + turn * (used - fixed)) % max(1, number_of - fixed)
        return jnp.zeros((number_of,), jnp.int32).at[order[jnp.where(places < fixed, places, moved)]].set(jnp.asarray(sizes, jnp.int32))

    sizes = jnp.where(number % 4 == 0, named(packed, number // 4), named(common, number - number // 4 - 1))
    mixed = jax.random.permutation(jax.random.fold_in(own, 3), number_of)
    donor, receiver = mixed[0:number_of // 2 * 2:2], mixed[1:number_of // 2 * 2:2]
    room = jnp.minimum(sizes[donor] - 1, bound - sizes[receiver]) // 2
    room = jnp.where((donor == order[0]) | (receiver == order[0]) | (sizes[receiver] == 0), 0, jnp.maximum(room, 0))
    moved = jax.random.randint(jax.random.fold_in(own, 4), (number_of // 2,), 0, 1 << 20) % (room + 1)
    sizes = sizes.at[donor].add(-moved).at[receiver].add(moved)
    items = jnp.searchsorted(jnp.cumsum(sizes), jnp.arange(rows * top), side="right").astype(jnp.int32)
    table = items.reshape(top, rows).T
    table = table[jax.random.permutation(jax.random.fold_in(own, 1), rows)]
    turn = jax.random.randint(jax.random.fold_in(own, 2), (rows, 1), 0, top)
    return jnp.take_along_axis(table, (jnp.arange(top)[None, :] + turn) % top, axis=1)


def shares(number_of, total, most, slope, full):
    weights = [(1 << 20) // math.isqrt(standing ** slope) + 1 for standing in range(1, number_of + 1)]
    largest = most if full else min(most, max(-(-total // number_of), total * weights[0] // sum(weights)))
    least = 1 if total - largest >= number_of - 1 else 0
    holding, surplus = [largest] + [least] * (number_of - 1), total - largest - least * (number_of - 1)
    while surplus > 0:
        movable = [i for i in range(1, number_of) if holding[i] < largest] or [i for i in range(1, number_of) if holding[i] < most]
        mass, budget = sum([weights[i] for i in movable]), surplus
        for i in movable:
            extra = min(most - holding[i], max(1, budget * weights[i] // mass), surplus)
            holding[i] = holding[i] + extra
            surplus = surplus - extra
    return np.array(holding)


def normal_values(stream_key, extent, scale, reach, cuts=(), held_as=jnp.bfloat16):
    factor_of = block_scale(stream_key, extent, cuts, -0.22, 0.18) if cuts else 1.0
    values = jax.random.normal(stream_key, extent, jnp.float32) * scale * factor_of
    return jnp.minimum(jnp.maximum(values, -reach), reach).astype(held_as)


def setup_inputs(seed: int = 0) -> dict:
    key_list = jax.random.split(jax.random.key(seed), 10)
    requests = normal_values(key_list[0], (TOKENS, D), 1.0, 6.0, ((0, 4), (1, 8)))
    expert_ids_keys = jax.random.split(jax.random.fold_in(key_list[1], 1), TOKENS // TOK_DEV)
    expert_ids_turns = jax.random.permutation(jax.random.fold_in(key_list[1], 3), TOKENS // TOK_DEV)
    expert_ids = jax.vmap(lambda own, number: assign_block(jax.random.fold_in(key_list[1], 2), own, number, TOK_DEV, EXPERTS, 2, CAP, 2))(expert_ids_keys, expert_ids_turns).reshape((TOKENS, 2))
    gate_values = jnp.clip(0.2 + 0.8 * jax.random.uniform(key_list[2], (TOKENS, 2), jnp.float32) ** block_scale(key_list[2], (TOKENS, 2), ((0, 4),), -0.2, 0.2), 0.2, 1.0)
    w_up = normal_values(key_list[3], (EXPERTS, D, HID), D ** -0.5, 0.15625, ((1, 4), (2, 8)))
    w_down = normal_values(key_list[4], (EXPERTS, D, HID), HID ** -0.5, 0.078125, ((1, 4), (2, 8)))
    tower_in = normal_values(key_list[5], (D, TASKS * TH), D ** -0.5, 0.15625, ((0, 8),))
    tower_bias = normal_values(key_list[6], (TASKS * TH,), 0.5, 3.0, (), jnp.float32)
    tower_out = normal_values(key_list[7], (TASKS, TH), TH ** -0.5, 0.375, (), jnp.float32)
    out_bias = normal_values(key_list[8], (TASKS,), 1.0, 3.0, (), jnp.float32)
    return {"requests": requests, "expert_ids": expert_ids, "gate_values": gate_values, "w_up": w_up, "w_down": w_down, "tower_in": tower_in, "tower_bias": tower_bias, "tower_out": tower_out, "out_bias": out_bias}


def slot_table(expert_ids):
    blocks = expert_ids.reshape(-1, TOK_DEV * 2)
    onehot = (blocks[:, :, None] == jnp.arange(EXPERTS, dtype=jnp.int32)[None, None, :]).astype(jnp.int32)
    before = jnp.cumsum(onehot, axis=1) - onehot
    slot_rank = jnp.sum(before * onehot, axis=2)
    return (blocks * CAP + slot_rank).reshape(-1, 2)


def reference(requests, expert_ids, gate_values, w_up, w_down, tower_in, tower_bias, tower_out, out_bias):
    slots = slot_table(expert_ids)
    nblocks = TOKENS // TOK_DEV
    block_of = jnp.arange(TOKENS, dtype=jnp.int32) // TOK_DEV
    flat_index = (block_of[:, None] * (EXPERTS * CAP) + slots).astype(jnp.int32)
    dispatched = jnp.zeros((nblocks * EXPERTS * CAP, D), jnp.bfloat16)
    dispatched = dispatched.at[flat_index.reshape(-1)].set(jnp.repeat(requests, 2, axis=0))
    grouped = dispatched.reshape(nblocks, EXPERTS, CAP, D).transpose(1, 0, 2, 3).reshape(EXPERTS, nblocks * CAP, D)
    groups_hid = N_TENSOR * N_REP
    width = HID // groups_hid

    def expert_ffn(operands):
        rows, up_mat, down_mat = operands
        hidden = jax.nn.relu(jnp.dot(rows, up_mat, preferred_element_type=jnp.float32)).astype(jnp.bfloat16)
        total = jnp.zeros((rows.shape[0], D), jnp.float32)
        for group in range(groups_hid):
            part = jnp.dot(hidden[:, group * width:(group + 1) * width],
                           down_mat[:, group * width:(group + 1) * width].T,
                           preferred_element_type=jnp.float32)
            rounded = lax.optimization_barrier(part.astype(jnp.bfloat16))
            total = total + rounded.astype(jnp.float32)
        return total.astype(jnp.bfloat16)

    expert_out = lax.map(expert_ffn, (grouped, w_up, w_down))
    back = expert_out.reshape(EXPERTS, nblocks, CAP, D).transpose(1, 0, 2, 3).reshape(nblocks * EXPERTS * CAP, D)
    first = back[flat_index[:, 0]].astype(jnp.float32)
    second = back[flat_index[:, 1]].astype(jnp.float32)
    mixed = (gate_values[:, 0:1] * first + gate_values[:, 1:2] * second).astype(jnp.bfloat16)
    pre = jnp.dot(mixed, tower_in, preferred_element_type=jnp.float32) + tower_bias[None, :]
    active = jax.nn.relu(pre).reshape(TOKENS, TASKS, TH)
    logits = jnp.sum(active * tower_out[None, :, :], axis=2) + out_bias[None, :]
    scores = jax.nn.sigmoid(logits).T
    return mixed, scores
```

```python
import jax
import jax.numpy as jnp
from jax import lax
from jax.experimental import pallas as pl
from jax.experimental.pallas import tpu as pltpu
from jax.sharding import PartitionSpec as P

ALL = ("expert", "tensor", "rep")
F32 = jnp.float32
BF16 = jnp.bfloat16


def tower_head(pre, tower_bias, tower_out, out_bias):
    active = jax.nn.relu(pre + tower_bias[None, :])
    active = active.reshape(pre.shape[0], tower_out.shape[0], tower_out.shape[1])
    logits = jnp.sum(active * tower_out[None, :, :], axis=2) + out_bias[None, :]
    return jax.nn.sigmoid(logits).T


def moved_weights(
    requests, expert_ids, gate_values, w_up, w_down, tower_in, tower_bias, tower_out, out_bias
):
    groups = lax.axis_size("expert")
    experts = w_up.shape[0]
    local_experts = experts // groups
    tok_rows = requests.shape[0]
    capacity = 3 * tok_rows // experts
    serve_up, serve_down = (
        lax.all_to_all(w_up, "expert", split_axis=0, concat_axis=1, tiled=True),
        lax.all_to_all(w_down, "expert", split_axis=0, concat_axis=1, tiled=True),
    )
    flat_ids = expert_ids.reshape(-1)
    onehot = (flat_ids[:, None] == jnp.arange(experts, dtype=jnp.int32)[None, :]).astype(jnp.int32)
    before = jnp.cumsum(onehot, axis=0) - onehot
    slot_rank = jnp.sum(before * onehot, axis=1)
    slots = (flat_ids * capacity + slot_rank).reshape(tok_rows, 2)
    slot_index = jnp.arange(experts * capacity, dtype=jnp.int32)
    spread = (
        (slot_index[:, None] == slots[None, :, 0]) | (slot_index[:, None] == slots[None, :, 1])
    ).astype(jnp.bfloat16)
    full_rows = lax.all_gather(requests, ("tensor", "rep"), axis=1, tiled=True)
    outgoing = jnp.dot(spread, full_rows, preferred_element_type=jnp.float32).astype(jnp.bfloat16)
    incoming = lax.all_to_all(outgoing, "expert", split_axis=0, concat_axis=0, tiled=True)
    shaped = incoming.reshape(groups, local_experts, capacity, incoming.shape[1])
    hidden_pre = jnp.einsum("secd,edh->sech", shaped, serve_up, preferred_element_type=jnp.float32)
    hidden = jax.nn.relu(hidden_pre).astype(jnp.bfloat16)
    partial_value = jnp.einsum(
        "sech,edh->secd", hidden, serve_down, preferred_element_type=jnp.float32
    )
    summed = lax.psum_scatter(
        partial_value.astype(jnp.bfloat16), ("tensor", "rep"), scatter_dimension=3, tiled=True
    ).astype(jnp.float32)
    expert_out = summed.astype(jnp.bfloat16).reshape(
        groups * local_experts * capacity, summed.shape[3]
    )
    returned = lax.all_to_all(expert_out, "expert", split_axis=0, concat_axis=0, tiled=True)
    pick_first = (slots[:, 0:1] == slot_index[None, :]).astype(jnp.bfloat16)
    pick_second = (slots[:, 1:2] == slot_index[None, :]).astype(jnp.bfloat16)
    first = jnp.dot(pick_first, returned, preferred_element_type=jnp.float32)
    second = jnp.dot(pick_second, returned, preferred_element_type=jnp.float32)
    mixed = (gate_values[:, 0:1] * first + gate_values[:, 1:2] * second).astype(jnp.bfloat16)
    pre = lax.psum_scatter(
        jnp.dot(mixed, tower_in, preferred_element_type=jnp.float32).astype(jnp.bfloat16),
        ("tensor", "rep"),
        scatter_dimension=0,
        tiled=True,
    ).astype(jnp.float32)
    scores = tower_head(pre, tower_bias, tower_out, out_bias)
    return (mixed, scores)


def permute(x, move):
    sizes = [lax.axis_size(a) for a in ALL]
    pairs = []
    for e in range(sizes[0]):
        for t in range(sizes[1]):
            for r in range(sizes[2]):
                e2, t2, r2 = move(e, t, r)
                pairs.append(
                    ((e * sizes[1] + t) * sizes[2] + r, (e2 * sizes[1] + t2) * sizes[2] + r2)
                )
    return lax.ppermute(x, ALL, pairs)


def gather_cols(packed, width):
    tail = packed[:, width:].astype(F32)
    ids = [tail[:, k : k + 1] for k in range(2)]
    gates = [
        tail[:, 2 + 3 * k : 3 + 3 * k]
        + tail[:, 3 + 3 * k : 4 + 3 * k]
        + tail[:, 4 + 3 * k : 5 + 3 * k]
        for k in range(2)
    ]
    return ids, gates


def up_kernel(place_ref, own_ref, other_ref, w_ref, *rest, width, blocks):
    outs, (xo_ref, xp_ref) = rest[:-2], rest[-2:]
    tok = own_ref.shape[1]
    experts, _, hid = w_ref.shape
    flip = place_ref[0]
    r = place_ref[1]
    for m in range(blocks):
        src = jnp.bitwise_xor(flip, m)
        xo_ref[m * tok : (m + 1) * tok, :] = own_ref[src]
        xp_ref[m * tok : (m + 1) * tok, :] = other_ref[src]
    ids, _ = gather_cols(xo_ref[...], width)
    xo = xo_ref[:, :width]
    xp = xp_ref[:, :width]
    tile = 256
    for n in range(0, hid, tile):
        parts = []
        for j in range(experts):
            wo = w_ref[j, pl.ds(pl.multiple_of(r * width, width), width), n : n + tile]
            wp = w_ref[j, pl.ds(pl.multiple_of((1 - r) * width, width), width), n : n + tile]
            parts.append(
                jnp.dot(xo, wo, preferred_element_type=F32)
                + jnp.dot(xp, wp, preferred_element_type=F32)
            )
        for k in range(2):
            acc = parts[experts - 1]
            for j in range(experts - 1):
                acc = jnp.where(ids[k] == float(j), parts[j], acc)
            acc = acc.astype(BF16)
            for m in range(blocks):
                outs[k * blocks + m][:, n : n + tile] = acc[m * tok : (m + 1) * tok, :]


def down_kernel(place_ref, own_ref, w_ref, *rest, width, blocks):
    hidden, (keep_ref, send_ref, y_ref) = rest[: 2 * blocks], rest[2 * blocks :]
    tok = own_ref.shape[1]
    experts = w_ref.shape[0]
    flip = place_ref[0]
    r = place_ref[1]
    packed = jnp.concatenate([own_ref[jnp.bitwise_xor(flip, m)] for m in range(blocks)], axis=0)
    ids, gates = gather_cols(packed, width)
    h = [
        jnp.concatenate([hidden[k * blocks + m][...] for m in range(blocks)], axis=0)
        for k in range(2)
    ]
    zero = jnp.zeros_like(h[0])
    keep = send = None
    for j in range(experts):
        hit = [ids[k] == float(j) for k in range(2)]
        rows = jnp.where(hit[0], h[0], jnp.where(hit[1], h[1], zero))
        gate = jnp.where(hit[0], gates[0], jnp.where(hit[1], gates[1], 0.0))
        nt = (((1,), (1,)), ((), ()))
        wk = w_ref[j, pl.ds(pl.multiple_of(r * width, width), width), :]
        ws = w_ref[j, pl.ds(pl.multiple_of((1 - r) * width, width), width), :]
        a = gate * lax.dot_general(rows, wk, nt, preferred_element_type=F32)
        b = gate * lax.dot_general(rows, ws, nt, preferred_element_type=F32)
        keep = a if keep is None else keep + a
        send = b if send is None else send + b
    for m in range(blocks):
        dst = jnp.bitwise_xor(flip, m)
        keep_ref[dst] = keep[m * tok : (m + 1) * tok, :].astype(BF16)
        send_ref[dst] = send[m * tok : (m + 1) * tok, :].astype(BF16)


VMEM = pl.BlockSpec(memory_space=pltpu.VMEM)
SMEM = pl.BlockSpec(memory_space=pltpu.SMEM)


def stationary(
    requests, expert_ids, gate_values, w_up, w_down, tower_in, tower_bias, tower_out, out_bias
):
    blocks = lax.axis_size("expert")
    tok, width = requests.shape
    hid = w_up.shape[2]
    e, t, r = (lax.axis_index(a) for a in ALL)
    place = jnp.stack([jnp.bitwise_xor(e, t), r]).astype(jnp.int32)

    def x_of(v):
        return permute(v, lambda e, t, r: (e ^ 1, t, r))

    def y_of(v):
        return permute(v, lambda e, t, r: (e ^ 2, t, r))

    def r_of(v):
        return permute(v, lambda e, t, r: (e, t, 1 - r))

    high = gate_values.astype(BF16)
    left = gate_values - high.astype(F32)
    mid = left.astype(BF16)
    low = (left - mid.astype(F32)).astype(BF16)
    cols = [requests, expert_ids.astype(BF16)]
    for k in range(2):
        cols += [v[:, k : k + 1] for v in (high, mid, low)]
    packed = jnp.concatenate(cols, axis=1)
    own = jnp.stack(
        [permute(packed, lambda e, t, r, k=k: (t, e ^ k, r)) for k in range(blocks)]
    )
    other = r_of(own)

    piece = jax.ShapeDtypeStruct((tok, hid), BF16)
    parts = pl.pallas_call(
        lambda *refs: up_kernel(*refs, width=width, blocks=blocks),
        out_shape=[piece] * (2 * blocks),
        in_specs=[SMEM, VMEM, VMEM, VMEM],
        out_specs=[VMEM] * (2 * blocks),
        scratch_shapes=[pltpu.VMEM((blocks * tok, packed.shape[1]), BF16)] * 2,
        name="up",
    )(place, own, other, w_up)
    (ao, an, ay, ad), (bo, bx, bn, bd) = parts[:blocks], parts[blocks:]

    rad, rbd = x_of(ad), y_of(bd)
    ran, rbn = x_of(an), y_of(bn)
    fa = (ay.astype(F32) + rad.astype(F32)).astype(BF16)
    fb = (bx.astype(F32) + rbd.astype(F32)).astype(BF16)
    ra2, rb2 = y_of(fa), x_of(fb)
    ha = jax.nn.relu(ao.astype(F32) + ran.astype(F32) + ra2.astype(F32)).astype(BF16)
    hb = jax.nn.relu(bo.astype(F32) + rbn.astype(F32) + rb2.astype(F32)).astype(BF16)

    hax, hay = x_of(ha), y_of(ha)
    hbx, hby = x_of(hb), y_of(hb)
    haxy, hbxy = x_of(hay), y_of(hbx)

    piece = jax.ShapeDtypeStruct((blocks, tok, width), BF16)
    keep, send = pl.pallas_call(
        lambda *refs: down_kernel(*refs, None, width=width, blocks=blocks),
        out_shape=[piece] * 2,
        in_specs=[SMEM] + [VMEM] * (2 + 2 * blocks),
        out_specs=[VMEM] * 2,
        name="down",
    )(place, own, w_down, ha, hax, hay, haxy, hb, hbx, hby, hbxy)

    back = r_of(send)
    both = (keep.astype(F32) + back.astype(F32)).astype(BF16)
    got = [permute(both[k], lambda e, t, r, k=k: (t ^ k, e, r)) for k in range(blocks)]
    mixed = sum(v.astype(F32) for v in got).astype(BF16)

    pre = jnp.dot(mixed, tower_in, preferred_element_type=F32).astype(BF16)
    reps = lax.axis_size("rep")
    pre = pre.reshape(blocks, reps, tok // blocks // reps, pre.shape[1])
    mine = lax.dynamic_index_in_dim(pre, r, 1, keepdims=False)
    theirs = lax.dynamic_index_in_dim(pre, 1 - r, 1, keepdims=False)
    half = (mine.astype(F32) + r_of(theirs).astype(F32)).astype(BF16)
    total = lax.dynamic_index_in_dim(half, t, 0, keepdims=False).astype(F32)
    for k in range(1, blocks):
        out = lax.dynamic_index_in_dim(half, jnp.bitwise_xor(t, k), 0, keepdims=False)
        total = total + permute(out, lambda e, t, r, k=k: (e, t ^ k, r)).astype(F32)
    scores = tower_head(total, tower_bias, tower_out, out_bias)
    return (mixed, scores)


def solution(mesh):
    groups, n_tensor, n_rep = (mesh.shape[a] for a in ALL)

    def per_device(*args):
        requests, w_up = args[0], args[3]
        rows = 2 * groups * requests.shape[0]
        fits = groups == n_tensor and groups == 2 * 2 and n_rep == 2 and w_up.shape[0] <= 256
        if fits and rows <= requests.shape[1] * n_tensor * n_rep:
            return stationary(*args)
        return moved_weights(*args)

    in_specs = (
        P("expert", ("tensor", "rep")),
        P("expert", None),
        P("expert", None),
        P(None, "expert", ("tensor", "rep")),
        P(None, "expert", ("tensor", "rep")),
        P(("tensor", "rep"), None),
        P(),
        P(),
        P(),
    )
    out_specs = (P("expert", ("tensor", "rep")), P(None, ("expert", "tensor", "rep")))
    return jax.shard_map(
        per_device, mesh=mesh, in_specs=in_specs, out_specs=out_specs, check_vma=False
    )
```

```python
import functools

import jax
import jax.numpy as jnp
from jax import lax
from jax.experimental import pallas as pl
from jax.experimental.pallas import tpu as pltpu
from jax.sharding import PartitionSpec as P


ALL = ("expert", "tensor", "rep")
F32 = jnp.float32
BF16 = jnp.bfloat16


def tower_head(pre, tower_bias, tower_out, out_bias):
    active = jax.nn.relu(pre + tower_bias[None, :])
    active = active.reshape(pre.shape[0], tower_out.shape[0], tower_out.shape[1])
    logits = jnp.sum(active * tower_out[None, :, :], axis=2) + out_bias[None, :]
    return jax.nn.sigmoid(logits).T


def moved_weights(
    requests, expert_ids, gate_values, w_up, w_down, tower_in, tower_bias, tower_out, out_bias
):
    groups = lax.axis_size("expert")
    experts = w_up.shape[0]
    local_experts = experts // groups
    tok_rows = requests.shape[0]
    capacity = 3 * tok_rows // experts
    serve_up, serve_down = (
        lax.all_to_all(w_up, "expert", split_axis=0, concat_axis=1, tiled=True),
        lax.all_to_all(w_down, "expert", split_axis=0, concat_axis=1, tiled=True),
    )
    flat_ids = expert_ids.reshape(-1)
    onehot = (flat_ids[:, None] == jnp.arange(experts, dtype=jnp.int32)[None, :]).astype(jnp.int32)
    before = jnp.cumsum(onehot, axis=0) - onehot
    slot_rank = jnp.sum(before * onehot, axis=1)
    slots = (flat_ids * capacity + slot_rank).reshape(tok_rows, 2)
    slot_index = jnp.arange(experts * capacity, dtype=jnp.int32)
    spread = (
        (slot_index[:, None] == slots[None, :, 0]) | (slot_index[:, None] == slots[None, :, 1])
    ).astype(jnp.bfloat16)
    full_rows = lax.all_gather(requests, ("tensor", "rep"), axis=1, tiled=True)
    outgoing = jnp.dot(spread, full_rows, preferred_element_type=jnp.float32).astype(jnp.bfloat16)
    incoming = lax.all_to_all(outgoing, "expert", split_axis=0, concat_axis=0, tiled=True)
    shaped = incoming.reshape(groups, local_experts, capacity, incoming.shape[1])
    hidden_pre = jnp.einsum("secd,edh->sech", shaped, serve_up, preferred_element_type=jnp.float32)
    hidden = jax.nn.relu(hidden_pre).astype(jnp.bfloat16)
    partial_value = jnp.einsum(
        "sech,edh->secd", hidden, serve_down, preferred_element_type=jnp.float32
    )
    summed = lax.psum_scatter(
        partial_value.astype(jnp.bfloat16), ("tensor", "rep"), scatter_dimension=3, tiled=True
    ).astype(jnp.float32)
    expert_out = summed.astype(jnp.bfloat16).reshape(
        groups * local_experts * capacity, summed.shape[3]
    )
    returned = lax.all_to_all(expert_out, "expert", split_axis=0, concat_axis=0, tiled=True)
    pick_first = (slots[:, 0:1] == slot_index[None, :]).astype(jnp.bfloat16)
    pick_second = (slots[:, 1:2] == slot_index[None, :]).astype(jnp.bfloat16)
    first = jnp.dot(pick_first, returned, preferred_element_type=jnp.float32)
    second = jnp.dot(pick_second, returned, preferred_element_type=jnp.float32)
    mixed = (gate_values[:, 0:1] * first + gate_values[:, 1:2] * second).astype(jnp.bfloat16)
    pre = lax.psum_scatter(
        jnp.dot(mixed, tower_in, preferred_element_type=jnp.float32).astype(jnp.bfloat16),
        ("tensor", "rep"),
        scatter_dimension=0,
        tiled=True,
    ).astype(jnp.float32)
    scores = tower_head(pre, tower_bias, tower_out, out_bias)
    return (mixed, scores)


def permute(x, move):
    sizes = [lax.axis_size(a) for a in ALL]
    pairs = []
    for e in range(sizes[0]):
        for t in range(sizes[1]):
            for r in range(sizes[2]):
                e2, t2, r2 = move(e, t, r)
                pairs.append(
                    ((e * sizes[1] + t) * sizes[2] + r, (e2 * sizes[1] + t2) * sizes[2] + r2)
                )
    return lax.ppermute(x, ALL, pairs)


NT = (((1,), (1,)), ((), ()))
LANES = 128
VMEM = pl.BlockSpec(memory_space=pltpu.VMEM)
PLAIN = pl.BlockSpec(memory_space=pltpu.VMEM)
SMEM = pl.BlockSpec(memory_space=pltpu.SMEM)
ANY = pl.BlockSpec(memory_space=pl.ANY)
SMALL = pltpu.CompilerParams(vmem_limit_bytes=20 << 20)
META = 16


def call(kernel, outs, operands, scratch=(), **static):
    specs, arrays = [], []
    for item in operands:
        spec, array = item if isinstance(item, tuple) else (VMEM, item)
        if spec is VMEM:
            array = pltpu.with_memory_space_constraint(array, pltpu.VMEM)
        specs.append(spec)
        arrays.append(array)
    return pl.pallas_call(
        functools.partial(kernel, **static),
        out_shape=[pltpu.VMEM(*o) for o in outs],
        in_specs=specs,
        out_specs=[VMEM] * len(outs),
        scratch_shapes=list(scratch),
        compiler_params=SMALL,
    )(*arrays)


def pack_kernel(req_ref, ids_ref, gates_ref, out_ref):
    width, tok = req_ref.shape
    out_ref[:width, :] = req_ref[...]
    gates = gates_ref[...]
    high = gates.astype(BF16).astype(F32)
    left = gates - high
    mid = left.astype(BF16).astype(F32)
    low = left - mid
    ids = ids_ref[...].astype(F32)
    fill = jnp.zeros((META - 8, tok), F32)
    out_ref[width:, :] = jnp.concatenate([ids, high, mid, low, fill], axis=0).astype(BF16)


def here():
    e, t, r = (lax.axis_index(name) for name in ALL)
    return jnp.bitwise_xor(e, t), t, r


def load_kernel(w_ref, out_ref, sem):
    copy = pltpu.make_async_copy(w_ref, out_ref, sem)
    copy.start()
    copy.wait()


def prepare_kernel(w_ref, mine_ref, other_ref, out_ref, tower_ref, sem):
    width = mine_ref.shape[0]
    _, _, r = here()
    copy = pltpu.make_async_copy(w_ref, out_ref, sem)
    copy.start()
    tower_ref[pl.ds(pl.multiple_of(r * width, width), width), :] = mine_ref[...]
    tower_ref[pl.ds(pl.multiple_of((1 - r) * width, width), width), :] = other_ref[...]
    copy.wait()


def fetch(own, other, so, sp, blocks, width):
    for k in range(blocks):
        so[k] = own[k][...]
        sp[k] = other[k][:width, :]


def arrange(so, sp, src, r, width, part):
    a, b = so[src, :width, :], sp[src]
    low = jnp.where(r == 0, a, b)
    high = jnp.where(r == 0, b, a)
    x = jnp.concatenate([low, high], axis=0).T
    cols = so[src, width:, :].astype(F32).T.astype(BF16)

    def order(v):
        groups = v.shape[0] // part
        pieces = [v[g * part : (g + 1) * part, :] for h in (0, 1) for g in range(h, groups, 2)]
        return jnp.concatenate(pieces, axis=0)

    return order(x), order(cols)


def project(x, cols, w_ref, acc, outs, tok):
    experts, _, hid = w_ref.shape
    tile = 2 * LANES
    for n in range(0, hid, tile):
        for j in range(experts):
            part = jnp.dot(x, w_ref[j, :, n : n + tile], preferred_element_type=F32).astype(BF16)
            for k in range(2):
                new = part
                if j:
                    hit = cols[:, k : k + 1] == jnp.asarray(j, BF16)
                    new = jnp.where(hit, part, acc[k])
                if j < experts - 1:
                    acc[k] = new
                else:
                    for m, out in enumerate(outs[k]):
                        out[:, n : n + tile] = new[m * tok : (m + 1) * tok, :]


def far_kernel(*refs, blocks, part):
    own, other, w_ref = refs[:blocks], refs[blocks : 2 * blocks], refs[2 * blocks]
    a_ref, b_ref, so, sp, acc = refs[2 * blocks + 1 :]
    width, tok = w_ref.shape[1] // 2, own[0].shape[1]
    flip, _, r = here()
    fetch(own, other, so, sp, blocks, width)
    x, cols = arrange(so, sp, jnp.bitwise_xor(flip, blocks - 1), r, width, part)
    project(x, cols, w_ref, acc, ([a_ref], [b_ref]), tok)


def near_kernel(*refs, blocks, part):
    own, other, w_ref = refs[:blocks], refs[blocks : 2 * blocks], refs[2 * blocks]
    near = blocks - 1
    outs, rest = refs[2 * blocks + 1 : 2 * blocks + 1 + 2 * near], refs[2 * blocks + 1 + 2 * near :]
    meta_ref, so, sp, acc, x = rest
    width, tok = w_ref.shape[1] // 2, own[0].shape[1]
    flip, _, r = here()
    fetch(own, other, so, sp, blocks, width)
    for m in range(blocks):
        rows, cols = arrange(so, sp, jnp.bitwise_xor(flip, m), r, width, part)
        if m < near:
            x[m * tok : (m + 1) * tok, :] = rows
        meta_ref[m * tok : (m + 1) * tok, :] = cols
    project(x[...], meta_ref[: near * tok, :], w_ref, acc, (outs[:near], outs[near:]), tok)


def down_kernel(*refs, blocks, mine):
    meta_ref, hidden, w_ref = refs[0], refs[1 : 1 + 2 * blocks], refs[1 + 2 * blocks]
    out_ref, h0, h1, mt = refs[2 + 2 * blocks :]
    experts = w_ref.shape[0]
    tok = hidden[0].shape[0]
    half = tok // 2
    _, _, r = here()
    side = r if mine else 1 - r
    for m in range(blocks):
        rows, at = slice(m * half, (m + 1) * half), pl.multiple_of(side * half, half)
        h0[rows, :] = hidden[m][pl.ds(at, half), :]
        h1[rows, :] = hidden[blocks + m][pl.ds(at, half), :]
        mt[rows, :] = meta_ref[pl.ds(pl.multiple_of(m * tok + at, half), half), :]
    meta = mt[...]
    gates = []
    for k in range(2):
        three = [meta[:, 2 * q + k : 2 * q + k + 1].astype(F32) for q in (1, 2, 3)]
        gates.append(three[0] + three[1] + three[2])
    ids = [meta[:, k : k + 1].astype(F32) for k in range(2)]
    zero = jnp.zeros(h0.shape, BF16)
    total = None
    for j in range(experts):
        first, second = (meta[:, k : k + 1] == jnp.asarray(j, BF16) for k in range(2))
        rows = jnp.where(first, h0[...], jnp.where(second, h1[...], zero))
        gate = jnp.where(ids[0] == float(j), gates[0], jnp.where(ids[1] == float(j), gates[1], 0.0))
        part = gate * lax.dot_general(rows, w_ref[j], NT, preferred_element_type=F32)
        total = part if total is None else total + part
    for m in range(blocks):
        out_ref[m] = total[m * half : (m + 1) * half, :].astype(BF16)


def add_kernel(a_ref, b_ref, *outs):
    for m, out in enumerate(outs):
        out[...] = (a_ref[m].astype(F32) + b_ref[m].astype(F32)).astype(BF16)


def route_kernel(*refs, blocks):
    pieces, outs, sp = refs[:blocks], refs[blocks : 2 * blocks], refs[2 * blocks]
    flip, _, _ = here()
    for m in range(blocks):
        sp[m] = pieces[m][...]
    for k in range(blocks):
        outs[k][...] = sp[jnp.bitwise_xor(flip, k)]


def tower_kernel(*refs, blocks):
    got, tower_ref = refs[:blocks], refs[blocks]
    mine_ref, theirs_ref = refs[blocks + 1 : blocks + 3]
    outs, pre = refs[blocks + 3 : 2 * blocks + 3], refs[2 * blocks + 3]
    _, t, r = here()
    width = mine_ref.shape[1]
    part = outs[0].shape[0]
    total = got[0][...].astype(F32)
    for g in got[1:]:
        total = total + g[...].astype(F32)
    mixed = total.astype(BF16)
    pre[...] = jnp.dot(mixed, tower_ref[...], preferred_element_type=F32)
    for k in range(blocks):
        at = pl.multiple_of(jnp.bitwise_xor(t, k) * part, part)
        outs[k][...] = pre[pl.ds(at, part), :].astype(BF16)
    low, high = mixed[:, :width], mixed[:, width:]
    mine_ref[...] = jnp.where(r == 0, low, high)
    theirs_ref[...] = jnp.where(r == 0, high, low)


def mixed_kernel(mine_ref, recv_ref, out_ref, both, *, part):
    _, _, r = here()
    for g in range(mine_ref.shape[0] // part):
        rows = slice(g * part, (g + 1) * part)
        both[pl.ds(pl.multiple_of((2 * g + r) * part, part), part), :] = mine_ref[rows, :]
        both[pl.ds(pl.multiple_of((2 * g + 1 - r) * part, part), part), :] = recv_ref[rows, :]
    out_ref[...] = both[...].T


def head_kernel(*refs, blocks):
    got, (bias_ref, tower_ref, last_ref, score_ref) = refs[:blocks], refs[blocks:]
    tasks, units = tower_ref.shape
    total = got[0][...].astype(F32)
    for g in got[1:]:
        total = total + g[...].astype(F32)
    rows = []
    for j in range(tasks):
        act = None
        for c in range(units // LANES):
            at = j * units + c * LANES
            pre = total[:, at : at + LANES] + bias_ref[at : at + LANES].reshape(1, LANES)
            one = jnp.maximum(pre, 0.0) * tower_ref[j : j + 1, c * LANES : (c + 1) * LANES]
            act = one if act is None else act + one
        rows.append(jnp.sum(act.T, axis=0, keepdims=True) + last_ref[0, j])
    score_ref[...] = jax.nn.sigmoid(jnp.concatenate(rows, axis=0))


def stationary(
    requests, expert_ids, gate_values, w_up, w_down, tower_in, tower_bias, tower_out, out_bias
):
    blocks, reps = lax.axis_size("expert"), lax.axis_size("rep")
    tok, width = requests.shape
    _, span, hid = w_up.shape
    units = tower_in.shape[1]
    part = tok // (blocks * reps)
    half = tok // reps

    def x_of(v):
        return permute(v, lambda e, t, r: (e ^ 1, t, r))

    def y_of(v):
        return permute(v, lambda e, t, r: (e ^ 2, t, r))

    def xy_of(v):
        return permute(v, lambda e, t, r: (e ^ 3, t, r))

    def z_of(v, k):
        return permute(v, lambda e, t, r: (e, t ^ k, r))

    def r_of(v):
        return permute(v, lambda e, t, r: (e, t, 1 - r))

    (packed,) = call(
        pack_kernel,
        [((width + META, tok), BF16)],
        [(PLAIN, v.T) for v in (requests, expert_ids, gate_values)],
    )
    own = [permute(packed, lambda e, t, r, k=k: (t, e ^ k, r)) for k in range(blocks)]
    one = [pltpu.SemaphoreType.DMA(())]
    (up,) = call(load_kernel, [(w_up.shape, BF16)], [(ANY, w_up)], one)
    other = [r_of(v) for v in own]

    slab = ((tok, hid), BF16)
    stage = [
        pltpu.VMEM((blocks, width + META, tok), BF16),
        pltpu.VMEM((blocks, width, tok), BF16),
    ]
    near = blocks - 1
    ad, bd = call(
        far_kernel,
        [slab] * 2,
        own + other + [up],
        stage + [pltpu.VMEM((2, tok, 2 * LANES), BF16)],
        blocks=blocks,
        part=part,
    )
    rad, rbd = x_of(ad), y_of(bd)
    *parts, meta = call(
        near_kernel,
        [slab] * (2 * near) + [((blocks * tok, META), BF16)],
        own + other + [up],
        stage
        + [
            pltpu.VMEM((2, near * tok, 2 * LANES), BF16),
            pltpu.VMEM((near * tok, span), BF16),
        ],
        blocks=blocks,
        part=part,
    )
    (ao, an, ay), (bo, bx, bn) = parts[:near], parts[near:]

    ran, rbn = x_of(an), y_of(bn)
    fa = (ay.astype(F32) + rad.astype(F32)).astype(BF16)
    fb = (bx.astype(F32) + rbd.astype(F32)).astype(BF16)
    ra2, rb2 = y_of(fa), x_of(fb)
    ha = jax.nn.relu(ao.astype(F32) + ran.astype(F32) + ra2.astype(F32)).astype(BF16)
    hb = jax.nn.relu(bo.astype(F32) + rbn.astype(F32) + rb2.astype(F32)).astype(BF16)

    hax, hay = x_of(ha), y_of(ha)
    hbx, hby = x_of(hb), y_of(hb)
    haxy, hbxy = x_of(hay), y_of(hbx)
    tower_other = r_of(tower_in)
    down, tower = call(
        prepare_kernel,
        [(w_down.shape, BF16), ((span, units), BF16)],
        [(ANY, w_down), (PLAIN, tower_in), tower_other],
        one,
    )

    cut = ((blocks, half, span), BF16)
    operands = [meta, ha, hax, hay, haxy, hb, hbx, hby, hbxy, down]
    scratch = [pltpu.VMEM((blocks * half, hid), BF16)] * 2
    scratch.append(pltpu.VMEM((blocks * half, META), BF16))
    (send,) = call(down_kernel, [cut], operands, scratch, blocks=blocks, mine=False)
    recv = r_of(send)
    (keep,) = call(down_kernel, [cut], operands, scratch, blocks=blocks, mine=True)
    slab = ((half, span), BF16)
    b0, b1, b2, b3 = call(add_kernel, [slab] * blocks, [keep, recv])
    p3 = xy_of(b3)
    pieces = [b0, x_of(b1), y_of(b2), p3]

    scratch = [pltpu.VMEM((blocks, half, span), BF16)]
    out = call(route_kernel, [slab] * blocks, pieces, scratch, blocks=blocks)
    got = [out[0]] + [z_of(out[k], k) for k in range(1, blocks)]
    mine, theirs, *pre = call(
        tower_kernel,
        [((half, width), BF16)] * 2 + [((part, units), BF16)] * blocks,
        got + [tower],
        [pltpu.VMEM((half, units), F32)],
        blocks=blocks,
    )
    got = [pre[0]] + [z_of(pre[k], k) for k in range(1, blocks)]
    recv = r_of(theirs)
    mixed = pl.pallas_call(
        functools.partial(mixed_kernel, part=part),
        out_shape=jax.ShapeDtypeStruct((width, tok), BF16),
        in_specs=[VMEM] * 2,
        out_specs=VMEM,
        scratch_shapes=[pltpu.VMEM((tok, width), BF16)],
        compiler_params=SMALL,
        name="mixed",
    )(*[pltpu.with_memory_space_constraint(v, pltpu.VMEM) for v in (mine, recv)])
    scores = pl.pallas_call(
        functools.partial(head_kernel, blocks=blocks),
        out_shape=jax.ShapeDtypeStruct((tower_out.shape[0], part), F32),
        in_specs=[VMEM] * (blocks + 2) + [SMEM],
        out_specs=VMEM,
        compiler_params=SMALL,
        name="head",
    )(
        *[pltpu.with_memory_space_constraint(v, pltpu.VMEM) for v in got + [tower_bias, tower_out]],
        out_bias.reshape(1, -1),
    )
    return (mixed.T, scores)


def solution(mesh):
    groups, n_tensor, n_rep = (mesh.shape[a] for a in ALL)

    def per_device(*args):
        requests, w_up = args[0], args[3]
        rows = 2 * groups * requests.shape[0]
        fits = groups == n_tensor and groups == 2 * 2 and n_rep == 2 and w_up.shape[0] <= 256
        fits = fits and requests.shape[0] == LANES
        if fits and rows <= requests.shape[1] * n_tensor * n_rep:
            return stationary(*args)
        return moved_weights(*args)

    in_specs = (
        P("expert", ("tensor", "rep")),
        P("expert", None),
        P("expert", None),
        P(None, "expert", ("tensor", "rep")),
        P(None, "expert", ("tensor", "rep")),
        P(("tensor", "rep"), None),
        P(),
        P(),
        P(),
    )
    out_specs = (P("expert", ("tensor", "rep")), P(None, ("expert", "tensor", "rep")))
    return jax.shard_map(
        per_device, mesh=mesh, in_specs=in_specs, out_specs=out_specs, check_vma=False
    )
```
